8 devices in a mesh: dp: 1 (over z), cy: 2 (over y), cx: 4 (over x, core).
Axes of the slice: x: 2, y: 2, z: 1, core: 2. Of those that a mesh axis runs over, the one named last changes fastest.
Arguments:
- query_rows: bfloat16 [16384, 12, 128], P(('dp', 'cy', 'cx'))
- key_rows: bfloat16 [16384, 2, 128], P(('dp', 'cy', 'cx'))
- value_rows: bfloat16 [16384, 2, 128], P(('dp', 'cy', 'cx'))
- out_rows: bfloat16 [16384, 12, 128], P(('dp', 'cy', 'cx'))
- grad_out: bfloat16 [16384, 12, 128], P(('dp', 'cy', 'cx'))
- log_sum_exp: float32 [16384, 12], P(('dp', 'cy', 'cx'))
Outputs:
- output 1: bfloat16 [16384, 12, 128], P(('dp', 'cy', 'cx'))
- output 2: bfloat16 [16384, 2, 128], P(('dp', 'cy', 'cx'))
- output 3: bfloat16 [16384, 2, 128], P(('dp', 'cy', 'cx'))
All inputs are finite; a program needn't handle non-finite values.
Results may differ from the reference program's by a relative error of at most 0.00636.
Values are sent between devices in bfloat16 or wider.
A program may use at most 1 GiB of HBM per device.

```python
import math
import jax
import jax.numpy as jnp
from jax import lax

Q_HEADS = 12
KV_HEADS = 2
HEAD_DIM = 128
TOK_DEV = 2048
CTX_DEVS = 8
ROW_BLOCK = 64
SEQ_LEN = CTX_DEVS * TOK_DEV
CHUNK_LEN = TOK_DEV // 2
GROUP_SIZE = Q_HEADS // KV_HEADS
N_BLOCKS = SEQ_LEN // ROW_BLOCK
SCALING = 1.0 / math.sqrt(HEAD_DIM)


def seq_positions():
    local_idx = jnp.arange(TOK_DEV, dtype=jnp.int32)
    dev_idx = jnp.arange(CTX_DEVS, dtype=jnp.int32)
    piece_id = jnp.where(local_idx[None, :] < CHUNK_LEN, dev_idx[:, None], 2 * CTX_DEVS - 1 - dev_idx[:, None])
    return (piece_id * CHUNK_LEN + local_idx[None, :] % CHUNK_LEN).reshape(SEQ_LEN)


def to_seq_order(row_data):
    split_rows = row_data.reshape((CTX_DEVS, 2, CHUNK_LEN) + row_data.shape[1:])
    return jnp.concatenate([split_rows[:, 0], split_rows[::-1, 1]], axis=0).reshape(row_data.shape)


def to_device_order(row_data):
    split_rows = row_data.reshape((2, CTX_DEVS, CHUNK_LEN) + row_data.shape[1:])
    return jnp.stack([split_rows[0], split_rows[1, ::-1]], axis=1).reshape(row_data.shape)


def forward_stats(q_seq, k_seq, v_seq):
    keys_f32 = k_seq.astype(jnp.float32)
    vals_f32 = v_seq.astype(jnp.float32)
    key_pos = jnp.arange(SEQ_LEN)
    q_blocks = q_seq.reshape(N_BLOCKS, ROW_BLOCK, KV_HEADS, GROUP_SIZE, HEAD_DIM)

    def one_block(block_in):
        q_blk, blk_idx = block_in
        query_pos = blk_idx * ROW_BLOCK + jnp.arange(ROW_BLOCK)
        keep_mask = (query_pos[:, None] >= key_pos[None, :])[None, None]
        scores = jnp.einsum('bkgd,skd->kgbs', q_blk.astype(jnp.float32), keys_f32) * SCALING
        masked = jnp.where(keep_mask, scores, -1e30)
        row_max = jnp.max(masked, axis=-1)
        exp_vals = jnp.exp(masked - row_max[..., None])
        row_sum = jnp.sum(exp_vals, axis=-1)
        prob_b16 = (exp_vals / row_sum[..., None]).astype(jnp.bfloat16)
        out_blk = jnp.einsum('kgbs,skd->bkgd', prob_b16.astype(jnp.float32), vals_f32)
        lse_blk = (row_max + jnp.log(row_sum)).transpose(2, 0, 1)
        return out_blk.astype(jnp.bfloat16).reshape(ROW_BLOCK, Q_HEADS, HEAD_DIM), lse_blk.reshape(ROW_BLOCK, Q_HEADS)

    out_blocks, lse_blocks = lax.map(one_block, (q_blocks, jnp.arange(N_BLOCKS)))
    return out_blocks.reshape(SEQ_LEN, Q_HEADS, HEAD_DIM), lse_blocks.reshape(SEQ_LEN, Q_HEADS)


def setup_inputs(seed: int = 0, part: int = 0) -> dict:
    root_key = jax.random.fold_in(jax.random.key(seed), part)
    sub_keys = jax.random.split(root_key, 6)
    shape_q = (SEQ_LEN, Q_HEADS, HEAD_DIM)
    shape_kv = (SEQ_LEN, KV_HEADS, HEAD_DIM)
    query_f32 = jax.random.normal(sub_keys[0], shape_q, jnp.float32)
    key_mean = jax.random.normal(sub_keys[1], (KV_HEADS, HEAD_DIM), jnp.float32)
    key_f32 = jax.random.normal(sub_keys[2], shape_kv, jnp.float32) + key_mean
    value_mean = jax.random.normal(sub_keys[3], (KV_HEADS, HEAD_DIM), jnp.float32)
    value_f32 = jax.random.normal(sub_keys[4], shape_kv, jnp.float32) + value_mean
    row_pos = seq_positions().astype(jnp.float32)
    dout_f32 = jax.random.normal(sub_keys[5], shape_q, jnp.float32) * jnp.sqrt((row_pos + 1.0) / 4.0)[:, None, None]
    query_rows = query_f32.astype(jnp.bfloat16)
    key_rows = key_f32.astype(jnp.bfloat16)
    value_rows = value_f32.astype(jnp.bfloat16)
    out_seq, lse_seq = forward_stats(to_seq_order(query_rows), to_seq_order(key_rows), to_seq_order(value_rows))
    return {'query_rows': query_rows, 'key_rows': key_rows, 'value_rows': value_rows, 'out_rows': to_device_order(out_seq), 'grad_out': dout_f32.astype(jnp.bfloat16), 'log_sum_exp': to_device_order(lse_seq)}


def reference(query_rows, key_rows, value_rows, out_rows, grad_out, log_sum_exp):
    q_seq = to_seq_order(query_rows)
    keys_f32 = to_seq_order(key_rows).astype(jnp.float32)
    vals_f32 = to_seq_order(value_rows).astype(jnp.float32)
    do_seq = to_seq_order(grad_out)
    delta_seq = jnp.einsum('shd,shd->sh', do_seq.astype(jnp.float32), to_seq_order(out_rows).astype(jnp.float32))
    lse_seq = to_seq_order(log_sum_exp)
    blk_shape = (N_BLOCKS, ROW_BLOCK, KV_HEADS, GROUP_SIZE)
    key_pos = jnp.arange(SEQ_LEN)

    def one_block(grad_acc, block_in):
        dk_acc, dv_acc = grad_acc
        q_blk, do_blk, lse_blk, delta_blk, blk_idx = block_in
        q_f32 = q_blk.astype(jnp.float32)
        do_f32 = do_blk.astype(jnp.float32)
        query_pos = blk_idx * ROW_BLOCK + jnp.arange(ROW_BLOCK)
        keep_mask = (query_pos[:, None] >= key_pos[None, :])[None, None]
        scores = jnp.einsum('bkgd,skd->kgbs', q_f32, keys_f32) * SCALING
        prob_f32 = jnp.where(keep_mask, jnp.exp(scores - lse_blk.transpose(1, 2, 0)[..., None]), 0.0)
        dprob_f32 = jnp.einsum('bkgd,skd->kgbs', do_f32, vals_f32)
        dscore = (prob_f32 * (dprob_f32 - delta_blk.transpose(1, 2, 0)[..., None])).astype(jnp.bfloat16).astype(jnp.float32)
        prob_rnd = prob_f32.astype(jnp.bfloat16).astype(jnp.float32)
        dq_blk = jnp.einsum('kgbs,skd->bkgd', dscore, keys_f32) * SCALING
        dk_acc = dk_acc + jnp.einsum('kgbs,bkgd->skd', dscore, q_f32)
        dv_acc = dv_acc + jnp.einsum('kgbs,bkgd->skd', prob_rnd, do_f32)
        return (dk_acc, dv_acc), dq_blk.astype(jnp.bfloat16).reshape(ROW_BLOCK, Q_HEADS, HEAD_DIM)

    zero_kv = jnp.zeros((SEQ_LEN, KV_HEADS, HEAD_DIM), jnp.float32)
    block_ins = (q_seq.reshape(blk_shape + (HEAD_DIM,)), do_seq.reshape(blk_shape + (HEAD_DIM,)), lse_seq.reshape(blk_shape), delta_seq.reshape(blk_shape), jnp.arange(N_BLOCKS))
    (dk_acc, dv_acc), dq_blocks = lax.scan(one_block, (zero_kv, zero_kv), block_ins)
    grad_query = to_device_order(dq_blocks.reshape(SEQ_LEN, Q_HEADS, HEAD_DIM))
    grad_key = to_device_order((dk_acc * SCALING).astype(jnp.bfloat16))
    grad_value = to_device_order(dv_acc.astype(jnp.bfloat16))
    return grad_query, grad_key, grad_value
```

```python
import functools
import math

import jax
import jax.numpy as jnp
from jax import lax
from jax.experimental import pallas as pl
from jax.experimental.pallas import tpu as pltpu
from jax.sharding import PartitionSpec as P

F32 = jnp.float32
BF16 = jnp.bfloat16
LANES = 128
SUB = 256


def split3(x):
    hi = lax.reduce_precision(x, 8, 7)
    mid = lax.reduce_precision(x - hi, 8, 7)
    return hi, mid, x - hi - mid


def dot_nn(a, b):
    return jnp.dot(a, b, preferred_element_type=F32)


def dot_nt(a, b):
    return lax.dot_general(a, b, (((1,), (1,)), ((), ())), preferred_element_type=F32)


def attn_kernel(cfg, *refs):
    local, half, scale, has_dq, has_dkv = cfg
    refs = list(refs)
    sel_ref = refs.pop(0)
    q_ref, qt_ref, do_ref, dot_ref, stat_ref, kv_ref, ones_ref = refs[:7]
    refs = refs[7:]
    dq_in = refs.pop(0) if has_dq else None
    dkv_in = refs.pop(0) if has_dkv else None
    dq_ref, dkv_ref, p_scr, ds_scr = refs
    d = q_ref.shape[-1]
    factor = scale * math.log2(math.e)

    @pl.when(pl.program_id(0) == 0)
    def _():
        dkv_ref[...] = dkv_in[...] if has_dkv else jnp.zeros_like(dkv_ref)

    dq_ref[...] = dq_in[...] if has_dq else jnp.zeros_like(dq_ref)

    def probs(qo, ko, width, row, keep):
        qs = pl.ds(qo + row, SUB)
        ks = pl.ds(ko, width)
        stat = stat_ref[0, qs, :]
        kt = jnp.concatenate([kv_ref[0:d, ks], ones_ref[0:LANES, 0:width]], axis=0)
        vt = jnp.concatenate([kv_ref[d : 2 * d, ks], ones_ref[LANES : 2 * LANES, 0:width]], axis=0)
        s = dot_nn(jnp.concatenate([q_ref[0, qs, :], stat], axis=1), kt)
        p = jnp.exp2(s * factor)
        if keep is not None:
            p = jnp.where(keep, p, 0.0)
        dp = dot_nn(jnp.concatenate([do_ref[0, qs, :], stat], axis=1), vt)
        rows = pl.ds(row, SUB)
        p_scr[rows, 0:width] = p.astype(BF16)
        ds_scr[rows, 0:width] = (p * dp).astype(BF16)

    def full_unit(qo, ko):
        for row in range(0, half, SUB):
            probs(qo, ko, half, row, None)
        qs = pl.ds(qo, half)
        ks = pl.ds(ko, half)
        p = p_scr[...]
        ds = ds_scr[...]
        dkv_ref[d : 2 * d, ks] += dot_nn(dot_ref[0, :, qs], p)
        dkv_ref[0:d, ks] += dot_nn(qt_ref[0, :, qs], ds)
        dq_ref[0, :, qs] += dot_nt(kv_ref[0:d, ks], ds)

    def diag_unit(off):
        for row in range(0, half, SUB):
            width = row + SUB
            shape = (SUB, width)
            keep = lax.broadcasted_iota(jnp.int32, shape, 0) + row >= lax.broadcasted_iota(jnp.int32, shape, 1)
            probs(off, off, width, row, keep)
        for col in range(0, half, SUB):
            qs = pl.ds(off + col, half - col)
            ks = pl.ds(off + col, SUB)
            p = p_scr[pl.ds(col, half - col), pl.ds(col, SUB)]
            ds = ds_scr[pl.ds(col, half - col), pl.ds(col, SUB)]
            dkv_ref[d : 2 * d, ks] += dot_nn(dot_ref[0, :, qs], p)
            dkv_ref[0:d, ks] += dot_nn(qt_ref[0, :, qs], ds)
        for row in range(0, half, SUB):
            ds = ds_scr[pl.ds(row, SUB), 0 : row + SUB]
            dq_ref[0, :, pl.ds(off + row, SUB)] += dot_nt(kv_ref[0:d, pl.ds(off, row + SUB)], ds)

    full_unit(half, 0)
    if local:
        diag_unit(0)
        diag_unit(half)
    else:
        off = pl.multiple_of(sel_ref[0] * half, half)
        full_unit(off, off)


def attn_step(sel, q, qt, do, dot, stat, kv, ones, dq, dkv, *, group, heads, local):
    d, tok = qt.shape[1], qt.shape[2]
    half = tok // 2
    first = group * heads
    row = pl.BlockSpec((1, tok, d), lambda h, s: (h + first, 0, 0))
    col = pl.BlockSpec((1, d, tok), lambda h, s: (h + first, 0, 0))
    own = pl.BlockSpec((1, d, tok), lambda h, s: (h, 0, 0))
    whole = lambda a: pl.BlockSpec(a.shape, lambda h, s: (0, 0))
    args = [sel, q, qt, do, dot, stat, kv, ones]
    in_specs = [row, col, row, col, row, whole(kv), whole(ones)]
    aliases = {}
    if dq is not None:
        aliases[len(args)] = 0
        args.append(dq)
        in_specs.append(own)
    if dkv is not None:
        aliases[len(args)] = 1
        args.append(dkv)
        in_specs.append(whole(dkv))
    cfg = (local, half, 1.0 / math.sqrt(d), dq is not None, dkv is not None)
    pairs = heads * half * half * 2
    return pl.pallas_call(
        functools.partial(attn_kernel, cfg),
        grid_spec=pltpu.PrefetchScalarGridSpec(
            num_scalar_prefetch=1,
            grid=(heads,),
            in_specs=in_specs,
            out_specs=[own, pl.BlockSpec((2 * d, tok), lambda h, s: (0, 0))],
            scratch_shapes=[pltpu.VMEM((half, half), BF16), pltpu.VMEM((half, half), BF16)],
        ),
        out_shape=[jax.ShapeDtypeStruct((heads, d, tok), F32), jax.ShapeDtypeStruct((2 * d, tok), F32)],
        input_output_aliases=aliases,
        compiler_params=pltpu.CompilerParams(vmem_limit_bytes=56 * 2**20),
        cost_estimate=pl.CostEstimate(flops=10 * pairs * d, bytes_accessed=heads * tok * d * 20, transcendentals=pairs),
        name="local_grads" if local else "step_grads",
    )(*args)


def solution(mesh):
    n_cx = mesh.shape["cx"]
    n_ctx = mesh.shape["cy"] * n_cx
    ctx_axes = ("cy", "cx")
    row_spec = P(("dp", "cy", "cx"), None, None)
    stat_spec = P(("dp", "cy", "cx"), None)
    ring = [r if r < n_cx else n_cx + (r - n_cx + n_cx // 2) % n_cx for r in range(n_ctx)] if n_cx == 4 else list(range(n_ctx))
    forward = [(ring[i], ring[(i + 1) % n_ctx]) for i in range(n_ctx)]
    backward = [(b, a) for a, b in forward]

    def local_grads(query_rows, key_rows, value_rows, out_rows, grad_out, log_sum_exp):
        tok, n_heads, d = query_rows.shape
        kv_heads = key_rows.shape[1]
        heads = n_heads // kv_heads
        half = tok // 2
        scale = 1.0 / math.sqrt(d)
        rank = lax.axis_index("cy") * n_cx + lax.axis_index("cx")
        ring_arr = jnp.array(ring, jnp.int32)
        pos = jnp.argmax(ring_arr == rank).astype(jnp.int32)

        q = query_rows.transpose(1, 0, 2)
        qt = query_rows.transpose(1, 2, 0)
        do = grad_out.transpose(1, 0, 2)
        dot = grad_out.transpose(1, 2, 0)
        delta = jnp.sum(grad_out.astype(F32) * out_rows.astype(F32), axis=-1)
        parts = [*split3(log_sum_exp / scale), *split3(delta)]
        lane = lax.broadcasted_iota(jnp.int32, (n_heads, tok, LANES), 2)
        stat = jnp.zeros((n_heads, tok, LANES), F32)
        for i, part in enumerate(parts):
            stat = jnp.where(lane == i, part.T[:, :, None], stat)
        stat = stat.astype(BF16)
        sub = lax.broadcasted_iota(jnp.int32, (2 * LANES, half), 0)
        minus = (sub < 3) | ((sub >= LANES + 3) & (sub < LANES + 6))
        ones = jnp.where(minus, -1.0, 0.0).astype(BF16)
        kt = key_rows.transpose(1, 2, 0)
        vt = value_rows.transpose(1, 2, 0)
        kv_own = [jnp.concatenate([kt[g], vt[g]], axis=0) for g in range(kv_heads)]

        perms = [forward if g % 2 == 0 else backward for g in range(kv_heads)]
        zero_sel = jnp.zeros((1,), jnp.int32)
        run = functools.partial(attn_step, q=q, qt=qt, do=do, dot=dot, stat=stat, ones=ones, heads=heads)
        dq = [None] * kv_heads
        own = [None] * kv_heads
        acc = [None] * kv_heads
        kv = list(kv_own)
        last = kv_heads - 1
        for g in range(last):
            dq[g], own[g] = run(zero_sel, kv=kv_own[g], dq=None, dkv=None, group=g, local=True)
        for t in range(1, n_ctx):
            for g in range(kv_heads):
                kv[g] = lax.ppermute(kv[g], ctx_axes, perms[g])
                shift = -t if g % 2 == 0 else t
                src = ring_arr[(pos + shift + n_ctx) % n_ctx]
                sel = (src > rank).astype(jnp.int32).reshape(1)
                if acc[g] is not None:
                    acc[g] = lax.ppermute(acc[g], ctx_axes, perms[g])
                dq[g], acc[g] = run(sel, kv=kv[g], dq=dq[g], dkv=acc[g], group=g, local=False)
        dq[last], own[last] = run(zero_sel, kv=kv_own[last], dq=dq[last], dkv=None, group=last, local=True)
        dks, dvs = [], []
        for g in range(kv_heads):
            total = lax.ppermute(acc[g], ctx_axes, perms[g]) + own[g]
            dks.append((total[:d] * scale).astype(BF16).T)
            dvs.append(total[d:].astype(BF16).T)
        grad_query = (jnp.concatenate(dq, axis=0) * scale).astype(BF16).transpose(2, 0, 1)
        return grad_query, jnp.stack(dks, axis=1), jnp.stack(dvs, axis=1)

    return jax.shard_map(local_grads, mesh=mesh, in_specs=(row_spec,) * 5 + (stat_spec,), out_specs=(row_spec,) * 3, check_vma=False)
```

```python
import functools
import math

import jax
import jax.numpy as jnp
from jax import lax
from jax.experimental import pallas as pl
from jax.experimental.pallas import tpu as pltpu
from jax.sharding import PartitionSpec as P

F32 = jnp.float32
BF16 = jnp.bfloat16
LANES = 128
SUB = 256
PARTS = 3
MESH = pl.DeviceIdType.MESH


def split3(x):
    hi = lax.reduce_precision(x, 8, 7)
    mid = lax.reduce_precision(x - hi, 8, 7)
    return hi, mid, x - hi - mid


def dot_nn(a, b):
    return jnp.dot(a, b, preferred_element_type=F32)


def dot_nt(a, b):
    return lax.dot_general(a, b, (((1,), (1,)), ((), ())), preferred_element_type=F32)


def ring_kernel(dims, q_hbm, do_hbm, stat_hbm, kv_own, dq_hbm, own_hbm, kv_hbm, dkv_hbm,
                q_v, do_v, qt_v, dot_v, stat_v, dq_v, kv_v, acc, tmp, p_scr, ds_scr,
                in_sem, stat_sem, out_sem, load_sem, tmp_sem, own_sem, kv_send, kv_recv, dkv_send, dkv_recv):
    n_cy, n_cx, groups, heads, tok, d = dims
    n = n_cy * n_cx
    half = tok // 2
    scale = 1.0 / math.sqrt(d)
    factor = scale * math.log2(math.e)
    dp = lax.axis_index("dp")
    rank = lax.axis_index("cy") * n_cx + lax.axis_index("cx")

    def ring(i):
        return i // n_cx * n_cx + (i % n_cx + n_cx // 2 * (i // n_cx)) % n_cx

    pos = ring(rank)
    targets = []
    for step in (1, n - 1):
        other = ring((pos + step) % n)
        targets.append((dp, other // n_cx, other % n_cx))

    def source_later(t, g):
        src = ring((pos + (n - t if g == 0 else t)) % n)
        return (src - rank + n - 1) // n

    barrier = pltpu.get_barrier_semaphore()
    for target in targets:
        pl.semaphore_signal(barrier, inc=1, device_id=target, device_id_type=MESH)
    pl.semaphore_wait(barrier, 2)

    def send_kv(g, t):
        src = kv_own.at[g] if isinstance(t, int) and t == 0 else kv_hbm.at[g, t - 1]
        return pltpu.make_async_remote_copy(src_ref=src, dst_ref=kv_hbm.at[g, t], send_sem=kv_send.at[g, t],
                                            recv_sem=kv_recv.at[g, t], device_id=targets[g], device_id_type=MESH)

    def wait_kv(g, t):
        slot = kv_hbm.at[g, t]
        pltpu.make_async_remote_copy(src_ref=slot, dst_ref=slot, send_sem=kv_send.at[g, t], recv_sem=kv_recv.at[g, t],
                                     device_id=targets[g], device_id_type=MESH).wait_recv()

    def send_dkv(g, t):
        return pltpu.make_async_remote_copy(src_ref=acc.at[g], dst_ref=dkv_hbm.at[g, t - 1], send_sem=dkv_send.at[g, t - 1],
                                            recv_sem=dkv_recv.at[g, t - 1], device_id=targets[g], device_id_type=MESH)

    def load_kv(g, t):
        return pltpu.make_async_copy(kv_hbm.at[g, t - 1], kv_v.at[g], load_sem.at[g])

    def load_own(g):
        return pltpu.make_async_copy(kv_own.at[g], kv_v.at[1 - g], load_sem.at[1 - g])

    def load_sum(g, t):
        return pltpu.make_async_copy(dkv_hbm.at[g, t - 1], tmp, tmp_sem)

    def store_own(g):
        return pltpu.make_async_copy(tmp, own_hbm.at[g], own_sem)

    def load_q(h):
        return pltpu.make_async_copy(q_hbm.at[h], q_v.at[h], in_sem.at[0, h])

    def load_do(h):
        return pltpu.make_async_copy(do_hbm.at[h], do_v.at[h], in_sem.at[1, h])

    def store_dq(h):
        return pltpu.make_async_copy(q_v.at[h], dq_hbm.at[h], out_sem.at[h])

    def terms(h, sums, kv):
        sub = lax.broadcasted_iota(jnp.int32, (LANES, SUB), 0) - h * (2 * PARTS)
        ones_l = jnp.where((sub >= 0) & (sub < PARTS), -1.0, 0.0).astype(BF16)
        ones_d = jnp.where((sub >= PARTS) & (sub < 2 * PARTS), -1.0, 0.0).astype(BF16)

        def probs(qo, ko, width, row, masked):
            qs = pl.ds(qo + row, SUB)
            ks = pl.ds(ko, width)
            stat = stat_v[qs, :]
            wide_l = jnp.concatenate([ones_l] * (width // SUB), axis=1)
            wide_d = jnp.concatenate([ones_d] * (width // SUB), axis=1)
            s = dot_nn(jnp.concatenate([q_v[h, qs, :], stat], axis=1), jnp.concatenate([kv[0:d, ks], wide_l], axis=0))
            p = jnp.exp2(s * factor)
            if masked:
                shape = (SUB, width)
                keep = lax.broadcasted_iota(jnp.int32, shape, 0) + row >= lax.broadcasted_iota(jnp.int32, shape, 1)
                p = jnp.where(keep, p, 0.0)
            dp_ = dot_nn(jnp.concatenate([do_v[h, qs, :], stat], axis=1), jnp.concatenate([kv[d : 2 * d, ks], wide_d], axis=0))
            rows = pl.ds(row, SUB)
            p_scr[rows, 0:width] = p.astype(BF16)
            ds_scr[rows, 0:width] = (p * dp_).astype(BF16)

        def full_unit(qo, ko, fresh=False):
            for row in range(0, half, SUB):
                probs(qo, ko, half, row, False)
            qs = pl.ds(qo, half)
            ks = pl.ds(ko, half)
            p = p_scr[...]
            ds = ds_scr[...]
            sums[d : 2 * d, ks] += dot_nn(dot_v[h, :, qs], p)
            sums[0:d, ks] += dot_nn(qt_v[h, :, qs], ds)
            dq = dot_nt(kv[0:d, ks], ds)
            if fresh:
                dq_v[h, :, qs] = dq
            else:
                dq_v[h, :, qs] += dq

        def diag_unit(off, fresh):
            for row in range(0, half, SUB):
                probs(off, off, row + SUB, row, True)
            for col in range(0, half, SUB):
                qs = pl.ds(off + col, half - col)
                ks = pl.ds(off + col, SUB)
                p = p_scr[pl.ds(col, half - col), pl.ds(col, SUB)]
                ds = ds_scr[pl.ds(col, half - col), pl.ds(col, SUB)]
                sums[d : 2 * d, ks] += dot_nn(dot_v[h, :, qs], p)
                sums[0:d, ks] += dot_nn(qt_v[h, :, qs], ds)
            for row in range(0, half, SUB):
                ds = ds_scr[pl.ds(row, SUB), 0 : row + SUB]
                dq = dot_nt(kv[0:d, pl.ds(off, row + SUB)], ds)
                if fresh:
                    dq_v[h, :, pl.ds(off + row, SUB)] = dq
                else:
                    dq_v[h, :, pl.ds(off + row, SUB)] += dq

        return full_unit, diag_unit

    def transposed(h):
        qt_v[h] = q_v[h].T
        dot_v[h] = do_v[h].T

    def finish(g):
        def body(i, carry):
            h = g * heads + i
            q_v[h] = (dq_v[h] * scale).astype(BF16).T
            store_dq(h).start()
            return carry
        lax.fori_loop(0, heads, body, 0)

    for g in range(groups):
        send_kv(g, 0).start()
    load_own(0).start()
    stat_copy = pltpu.make_async_copy(stat_hbm, stat_v, stat_sem)
    stat_copy.start()

    def load_head(h, carry):
        load_q(h).start()
        load_do(h).start()
        return carry
    lax.fori_loop(0, groups * heads, load_head, 0)
    tmp[...] = jnp.zeros_like(tmp)
    stat_copy.wait()
    load_own(0).wait()

    def own_first(h, carry):
        load_q(h).wait()
        load_do(h).wait()
        transposed(h)
        full_unit, diag_unit = terms(h, tmp, kv_v.at[1])
        full_unit(half, 0, fresh=True)
        diag_unit(0, True)
        diag_unit(half, False)

        @pl.when(h == heads // 2)
        def _():
            wait_kv(0, 0)
            send_kv(0, 1).start()
            load_kv(0, 1).start()
        return carry
    lax.fori_loop(0, heads, own_first, 0)
    store_own(0).start()

    def ring_step(t, carry):
        for g in range(groups):
            load_kv(g, t).wait()
            sel = source_later(t, g)
            off = pl.multiple_of(sel * half, half)

            @pl.when(t >= 2)
            def _():
                send_dkv(g, t - 1).wait_send()
            acc[g] = jnp.zeros((2 * d, tok), F32)

            if g == 0:
                wait_kv(1, t - 1)

                @pl.when(t < n - 1)
                def _():
                    send_kv(1, t).start()
                load_kv(1, t).start()
            else:
                @pl.when(t < n - 1)
                def _():
                    wait_kv(0, t)
                    load_kv(0, t + 1).start()

                @pl.when(t < n - 2)
                def _():
                    send_kv(0, t + 1).start()

                @pl.when(t == n - 1)
                def _():
                    load_own(1).start()

            def head(i, c):
                h = g * heads + i
                if g == 1:
                    @pl.when(t == 1)
                    def _():
                        load_q(h).wait()
                        load_do(h).wait()
                        transposed(h)
                        dq_v[h] = jnp.zeros((d, tok), F32)
                full_unit, _ = terms(h, acc.at[g], kv_v.at[g])
                full_unit(half, 0)
                full_unit(off, off)

                @pl.when((i == heads - 2) & (t >= 2))
                def _():
                    if g == 0:
                        @pl.when(t == 2)
                        def _():
                            store_own(0).wait()
                    send_dkv(g, t - 1).wait_recv()
                    load_sum(g, t - 1).start()
                return c
            lax.fori_loop(0, heads, head, 0)

            @pl.when(t >= 2)
            def _():
                load_sum(g, t - 1).wait()
                acc[g] += tmp[...]
            send_dkv(g, t).start()
        return carry
    lax.fori_loop(1, n, ring_step, 0)

    finish(0)
    tmp[...] = jnp.zeros_like(tmp)
    load_own(1).wait()

    def own_last(i, carry):
        h = heads + i
        full_unit, diag_unit = terms(h, tmp, kv_v.at[0])
        full_unit(half, 0)
        diag_unit(0, False)
        diag_unit(half, False)
        return carry
    lax.fori_loop(0, heads, own_last, 0)
    store_own(1).start()
    finish(1)

    def sent(t, carry):
        for g in range(groups):
            send_kv(g, t).wait_send()
        return carry
    for g in range(groups):
        send_kv(g, 0).wait_send()
    lax.fori_loop(1, n - 1, sent, 0)
    for g in range(groups):
        send_dkv(g, n - 1).wait_send()
        send_dkv(g, n - 1).wait_recv()
    store_own(1).wait()

    def stored(h, carry):
        store_dq(h).wait()
        return carry
    lax.fori_loop(0, groups * heads, stored, 0)


def ring_grads(q, do, stat, kv, dims):
    n_cy, n_cx, groups, heads, tok, d = dims
    n = n_cy * n_cx
    half = tok // 2
    hbm = pl.BlockSpec(memory_space=pl.ANY)
    dma = pltpu.SemaphoreType.DMA
    all_heads = groups * heads
    vmem = pltpu.VMEM
    return pl.pallas_call(
        functools.partial(ring_kernel, dims),
        in_specs=[hbm] * 4,
        out_specs=[hbm] * 4,
        out_shape=[
            jax.ShapeDtypeStruct((all_heads, tok, d), BF16),
            jax.ShapeDtypeStruct((groups, 2 * d, tok), F32),
            jax.ShapeDtypeStruct((groups, n - 1, 2 * d, tok), BF16),
            jax.ShapeDtypeStruct((groups, n - 1, 2 * d, tok), F32),
        ],
        scratch_shapes=[
            vmem((all_heads, tok, d), BF16), vmem((all_heads, tok, d), BF16),
            vmem((all_heads, d, tok), BF16), vmem((all_heads, d, tok), BF16),
            vmem((tok, LANES), BF16), vmem((all_heads, d, tok), F32),
            vmem((groups, 2 * d, tok), BF16), vmem((groups, 2 * d, tok), F32), vmem((2 * d, tok), F32),
            vmem((half, half), BF16), vmem((half, half), BF16),
            dma((2, all_heads)), dma, dma((all_heads,)), dma((groups,)), dma, dma,
            dma((groups, n - 1)), dma((groups, n - 1)), dma((groups, n - 1)), dma((groups, n - 1)),
        ],
        compiler_params=pltpu.CompilerParams(vmem_limit_bytes=67043328, collective_id=0, has_side_effects=True),
        name="ring_grads",
    )(q, do, stat, kv)


def solution(mesh):
    n_cy, n_cx = mesh.shape["cy"], mesh.shape["cx"]
    row_spec = P(("dp", "cy", "cx"), None, None)
    stat_spec = P(("dp", "cy", "cx"), None)

    def local_grads(query_rows, key_rows, value_rows, out_rows, grad_out, log_sum_exp):
        tok, n_heads, d = query_rows.shape
        groups = key_rows.shape[1]
        heads = n_heads // groups
        scale = 1.0 / math.sqrt(d)
        delta = jnp.sum(grad_out.astype(F32) * out_rows.astype(F32), axis=-1)
        parts = jnp.stack([*split3(log_sum_exp / scale), *split3(delta)], axis=-1).reshape(tok, 2 * PARTS * n_heads)
        stat = jnp.pad(parts, ((0, 0), (0, LANES - 2 * PARTS * n_heads))).astype(BF16)
        kv = jnp.concatenate([key_rows.transpose(1, 2, 0), value_rows.transpose(1, 2, 0)], axis=1)
        dims = (n_cy, n_cx, groups, heads, tok, d)
        dq, own, _, sums = ring_grads(query_rows.transpose(1, 0, 2), grad_out.transpose(1, 0, 2), stat, kv, dims)
        total = sums[:, -1] + own
        grad_key = (total[:, :d] * scale).astype(BF16).transpose(2, 0, 1)
        grad_value = total[:, d:].astype(BF16).transpose(2, 0, 1)
        return dq.transpose(1, 0, 2), grad_key, grad_value

    return jax.shard_map(local_grads, mesh=mesh, in_specs=(row_spec,) * 5 + (stat_spec,), out_specs=(row_spec,) * 3, check_vma=False)
```

```python
import functools
import math

import jax
import jax.numpy as jnp
from jax import lax
from jax.experimental import pallas as pl
from jax.experimental.pallas import tpu as pltpu
from jax.sharding import PartitionSpec as P

F32 = jnp.float32
BF16 = jnp.bfloat16
LANES = 128
SUB = 256
PARTS = 3
MESH = pl.DeviceIdType.MESH


def split3(x):
    hi = lax.reduce_precision(x, 8, 7)
    mid = lax.reduce_precision(x - hi, 8, 7)
    return hi, mid, x - hi - mid


def dot_nn(a, b):
    return jnp.dot(a, b, preferred_element_type=F32)


def dot_nt(a, b):
    return lax.dot_general(a, b, (((1,), (1,)), ((), ())), preferred_element_type=F32)


def ring_kernel(dims, q_hbm, do_hbm, stat_hbm, kv_own, dq_hbm, own_hbm, kv_hbm, dkv_hbm,
                q_v, do_v, qt_v, dot_v, stat_v, dq_v, kv_v, acc, tmp, p_scr, ds_scr,
                in_sem, stat_sem, out_sem, load_sem, tmp_sem, own_sem, kv_send, kv_recv, dkv_send, dkv_recv):
    n_cy, n_cx, groups, heads, tok, d = dims
    n = n_cy * n_cx
    half = tok // 2
    scale = 1.0 / math.sqrt(d)
    factor = scale * math.log2(math.e)
    dp = lax.axis_index("dp")
    rank = lax.axis_index("cy") * n_cx + lax.axis_index("cx")

    def ring(i):
        return i // n_cx * n_cx + (i % n_cx + n_cx // 2 * (i // n_cx)) % n_cx

    pos = ring(rank)
    targets = []
    for step in (1, n - 1):
        other = ring((pos + step) % n)
        targets.append((dp, other // n_cx, other % n_cx))

    def source_later(t, g):
        src = ring((pos + (n - t if g == 0 else t)) % n)
        return (src - rank + n - 1) // n

    barrier = pltpu.get_barrier_semaphore()
    for target in targets:
        pl.semaphore_signal(barrier, inc=1, device_id=target, device_id_type=MESH)
    pl.semaphore_wait(barrier, 2)

    def send_kv(g, t):
        src = kv_own.at[g] if isinstance(t, int) and t == 0 else kv_hbm.at[g, t - 1]
        return pltpu.make_async_remote_copy(src_ref=src, dst_ref=kv_hbm.at[g, t], send_sem=kv_send.at[g, t],
                                            recv_sem=kv_recv.at[g, t], device_id=targets[g], device_id_type=MESH)

    def wait_kv(g, t):
        slot = kv_hbm.at[g, t]
        pltpu.make_async_remote_copy(src_ref=slot, dst_ref=slot, send_sem=kv_send.at[g, t], recv_sem=kv_recv.at[g, t],
                                     device_id=targets[g], device_id_type=MESH).wait_recv()

    def send_dkv(g, t):
        return pltpu.make_async_remote_copy(src_ref=acc.at[g], dst_ref=dkv_hbm.at[g, t - 1], send_sem=dkv_send.at[g, t - 1],
                                            recv_sem=dkv_recv.at[g, t - 1], device_id=targets[g], device_id_type=MESH)

    def load_kv(g, t):
        return pltpu.make_async_copy(kv_hbm.at[g, t - 1], kv_v.at[g], load_sem.at[g])

    def load_own(g):
        return pltpu.make_async_copy(kv_own.at[g], kv_v.at[1 - g], load_sem.at[1 - g])

    def load_sum(g, t):
        return pltpu.make_async_copy(dkv_hbm.at[g, t - 1], tmp, tmp_sem)

    def store_own(g):
        return pltpu.make_async_copy(tmp, own_hbm.at[g], own_sem)

    def load_q(h):
        return pltpu.make_async_copy(q_hbm.at[h], q_v.at[h], in_sem.at[0, h])

    def load_do(h):
        return pltpu.make_async_copy(do_hbm.at[h], do_v.at[h], in_sem.at[1, h])

    def store_dq(h):
        return pltpu.make_async_copy(q_v.at[h], dq_hbm.at[h], out_sem.at[h])

    def terms(h, sums, kv):
        sub = lax.broadcasted_iota(jnp.int32, (LANES, SUB), 0) - h * (2 * PARTS)
        ones_l = jnp.where((sub >= 0) & (sub < PARTS), -1.0, 0.0).astype(BF16)
        ones_d = jnp.where((sub >= PARTS) & (sub < 2 * PARTS), -1.0, 0.0).astype(BF16)

        def probs(qo, ko, width, row, masked):
            qs = pl.ds(qo + row, SUB)
            ks = pl.ds(ko, width)
            stat = stat_v[qs, :]
            wide_l = jnp.concatenate([ones_l] * (width // SUB), axis=1)
            wide_d = jnp.concatenate([ones_d] * (width // SUB), axis=1)
            s = dot_nn(jnp.concatenate([q_v[h, qs, :], stat], axis=1), jnp.concatenate([kv[0:d, ks], wide_l], axis=0))
            p = jnp.exp2(s * factor)
            if masked:
                shape = (SUB, width)
                keep = lax.broadcasted_iota(jnp.int32, shape, 0) + row >= lax.broadcasted_iota(jnp.int32, shape, 1)
                p = jnp.where(keep, p, 0.0)
            dp_ = dot_nn(jnp.concatenate([do_v[h, qs, :], stat], axis=1), jnp.concatenate([kv[d : 2 * d, ks], wide_d], axis=0))
            rows = pl.ds(row, SUB)
            p_scr[rows, 0:width] = p.astype(BF16)
            ds_scr[rows, 0:width] = (p * dp_).astype(BF16)

        def full_unit(qo, ko, fresh=False):
            for row in range(0, half, SUB):
                probs(qo, ko, half, row, False)
            qs = pl.ds(qo, half)
            ks = pl.ds(ko, half)
            p = p_scr[...]
            ds = ds_scr[...]
            sums[d : 2 * d, ks] += dot_nn(dot_v[h, :, qs], p)
            sums[0:d, ks] += dot_nn(qt_v[h, :, qs], ds)
            dq = dot_nt(kv[0:d, ks], ds)
            if fresh:
                dq_v[h, :, qs] = dq
            else:
                dq_v[h, :, qs] += dq

        def diag_unit(off, fresh):
            for row in range(0, half, SUB):
                probs(off, off, row + SUB, row, True)
            for col in range(0, half, SUB):
                qs = pl.ds(off + col, half - col)
                ks = pl.ds(off + col, SUB)
                p = p_scr[pl.ds(col, half - col), pl.ds(col, SUB)]
                ds = ds_scr[pl.ds(col, half - col), pl.ds(col, SUB)]
                sums[d : 2 * d, ks] += dot_nn(dot_v[h, :, qs], p)
                sums[0:d, ks] += dot_nn(qt_v[h, :, qs], ds)
            for row in range(0, half, SUB):
                ds = ds_scr[pl.ds(row, SUB), 0 : row + SUB]
                dq = dot_nt(kv[0:d, pl.ds(off, row + SUB)], ds)
                if fresh:
                    dq_v[h, :, pl.ds(off + row, SUB)] = dq
                else:
                    dq_v[h, :, pl.ds(off + row, SUB)] += dq

        return full_unit, diag_unit

    def transposed(h):
        qt_v[h] = q_v[h].T
        dot_v[h] = do_v[h].T

    def finish(g):
        def body(i, carry):
            h = g * heads + i
            q_v[h] = (dq_v[h] * scale).astype(BF16).T
            store_dq(h).start()
            return carry
        lax.fori_loop(0, heads, body, 0)

    for g in range(groups):
        send_kv(g, 0).start()
    load_own(0).start()
    stat_copy = pltpu.make_async_copy(stat_hbm, stat_v, stat_sem)
    stat_copy.start()

    def load_head(h, carry):
        for g in range(groups):
            load_q(g * heads + h).start()
            load_do(g * heads + h).start()
        return carry
    lax.fori_loop(0, heads, load_head, 0)
    tmp[...] = jnp.zeros_like(tmp)
    stat_copy.wait()
    load_own(0).wait()

    def own_first(h, carry):
        for g in range(groups):
            load_q(g * heads + h).wait()
            load_do(g * heads + h).wait()
            transposed(g * heads + h)
        dq_v[heads + h] = jnp.zeros((d, tok), F32)
        full_unit, diag_unit = terms(h, tmp, kv_v.at[1])
        full_unit(half, 0, fresh=True)
        diag_unit(0, True)
        diag_unit(half, False)

        @pl.when(h == heads // 2)
        def _():
            wait_kv(0, 0)
            send_kv(0, 1).start()
            load_kv(0, 1).start()
        return carry
    lax.fori_loop(0, heads, own_first, 0)
    store_own(0).start()

    def ring_step(t, carry):
        for g in range(groups):
            load_kv(g, t).wait()
            sel = source_later(t, g)
            off = pl.multiple_of(sel * half, half)

            @pl.when(t >= 2)
            def _():
                send_dkv(g, t - 1).wait_send()
            acc[g] = jnp.zeros((2 * d, tok), F32)

            if g == 0:
                wait_kv(1, t - 1)

                @pl.when(t < n - 1)
                def _():
                    send_kv(1, t).start()
                load_kv(1, t).start()
            else:
                @pl.when(t < n - 1)
                def _():
                    wait_kv(0, t)
                    load_kv(0, t + 1).start()

                @pl.when(t < n - 2)
                def _():
                    send_kv(0, t + 1).start()

                @pl.when(t == n - 1)
                def _():
                    load_own(1).start()

            def head(i, c):
                h = g * heads + i
                full_unit, _ = terms(h, acc.at[g], kv_v.at[g])
                full_unit(half, 0)
                full_unit(off, off)

                @pl.when((i == heads - 2) & (t >= 2))
                def _():
                    if g == 0:
                        @pl.when(t == 2)
                        def _():
                            store_own(0).wait()
                    send_dkv(g, t - 1).wait_recv()
                    load_sum(g, t - 1).start()
                return c
            lax.fori_loop(0, heads, head, 0)

            @pl.when(t >= 2)
            def _():
                load_sum(g, t - 1).wait()
                acc[g] += tmp[...]
            send_dkv(g, t).start()
        return carry
    lax.fori_loop(1, n, ring_step, 0)

    finish(0)
    tmp[...] = jnp.zeros_like(tmp)
    load_own(1).wait()

    def own_last(i, carry):
        h = heads + i
        full_unit, diag_unit = terms(h, tmp, kv_v.at[0])
        full_unit(half, 0)
        diag_unit(0, False)
        diag_unit(half, False)
        return carry
    lax.fori_loop(0, heads, own_last, 0)
    store_own(1).start()
    finish(1)

    def sent(t, carry):
        for g in range(groups):
            send_kv(g, t).wait_send()
        return carry
    for g in range(groups):
        send_kv(g, 0).wait_send()
    lax.fori_loop(1, n - 1, sent, 0)
    for g in range(groups):
        send_dkv(g, n - 1).wait_send()
        send_dkv(g, n - 1).wait_recv()
    store_own(1).wait()

    def stored(h, carry):
        store_dq(h).wait()
        return carry
    lax.fori_loop(0, groups * heads, stored, 0)


def ring_grads(q, do, stat, kv, dims):
    n_cy, n_cx, groups, heads, tok, d = dims
    n = n_cy * n_cx
    half = tok // 2
    hbm = pl.BlockSpec(memory_space=pl.ANY)
    dma = pltpu.SemaphoreType.DMA
    all_heads = groups * heads
    vmem = pltpu.VMEM
    return pl.pallas_call(
        functools.partial(ring_kernel, dims),
        in_specs=[hbm] * 4,
        out_specs=[hbm] * 4,
        out_shape=[
            jax.ShapeDtypeStruct((all_heads, tok, d), BF16),
            jax.ShapeDtypeStruct((groups, 2 * d, tok), F32),
            jax.ShapeDtypeStruct((groups, n - 1, 2 * d, tok), BF16),
            jax.ShapeDtypeStruct((groups, n - 1, 2 * d, tok), F32),
        ],
        scratch_shapes=[
            vmem((all_heads, tok, d), BF16), vmem((all_heads, tok, d), BF16),
            vmem((all_heads, d, tok), BF16), vmem((all_heads, d, tok), BF16),
            vmem((tok, LANES), BF16), vmem((all_heads, d, tok), F32),
            vmem((groups, 2 * d, tok), BF16), vmem((groups, 2 * d, tok), F32), vmem((2 * d, tok), F32),
            vmem((half, half), BF16), vmem((half, half), BF16),
            dma((2, all_heads)), dma, dma((all_heads,)), dma((groups,)), dma, dma,
            dma((groups, n - 1)), dma((groups, n - 1)), dma((groups, n - 1)), dma((groups, n - 1)),
        ],
        compiler_params=pltpu.CompilerParams(vmem_limit_bytes=67043328, collective_id=0, has_side_effects=True),
        name="ring_grads",
    )(q, do, stat, kv)


def solution(mesh):
    n_cy, n_cx = mesh.shape["cy"], mesh.shape["cx"]
    row_spec = P(("dp", "cy", "cx"), None, None)
    stat_spec = P(("dp", "cy", "cx"), None)

    def local_grads(query_rows, key_rows, value_rows, out_rows, grad_out, log_sum_exp):
        tok, n_heads, d = query_rows.shape
        groups = key_rows.shape[1]
        heads = n_heads // groups
        scale = 1.0 / math.sqrt(d)
        delta = jnp.sum(grad_out.astype(F32) * out_rows.astype(F32), axis=-1)
        parts = jnp.stack([*split3(log_sum_exp / scale), *split3(delta)], axis=-1).reshape(tok, 2 * PARTS * n_heads)
        stat = jnp.pad(parts, ((0, 0), (0, LANES - 2 * PARTS * n_heads))).astype(BF16)
        kv = jnp.concatenate([key_rows.transpose(1, 2, 0), value_rows.transpose(1, 2, 0)], axis=1)
        dims = (n_cy, n_cx, groups, heads, tok, d)
        dq, own, _, sums = ring_grads(query_rows.transpose(1, 0, 2), grad_out.transpose(1, 0, 2), stat, kv, dims)
        total = sums[:, -1] + own
        grad_key = (total[:, :d] * scale).astype(BF16).transpose(2, 0, 1)
        grad_value = total[:, d:].astype(BF16).transpose(2, 0, 1)
        return dq.transpose(1, 0, 2), grad_key, grad_value

    return jax.shard_map(local_grads, mesh=mesh, in_specs=(row_spec,) * 5 + (stat_spec,), out_specs=(row_spec,) * 3, check_vma=False)
```
